32 devices in a mesh: dp: 4 (over y, x), expert: 8 (over z, core).
Axes of the slice: x: 2, y: 2, z: 4, core: 2. Of those that a mesh axis runs over, the one named last changes fastest.
Arguments:
- shortcut_in: bfloat16 [128, 7168], P('expert', 'dp'), may hold values from -6 to 6
- current_in: bfloat16 [128, 7168], P('expert', 'dp'), may hold values from -6 to 6
- expert_ids: int32 [128, 4], P('expert'), may hold values from 0 to 7, all different within a row; in each aligned block of 16 rows (0 to 15, 16 to 31, ...) at most 12 rows name the same one
- route_weight: float32 [128, 4], P('expert'), may hold values from 0.1 to 1
- gate_weight: bfloat16 [8, 7168, 2048], P('expert', 'dp'), may hold values from -0.09375 to 0.09375
- up_weight: bfloat16 [8, 7168, 2048], P('expert', 'dp'), may hold values from -0.09375 to 0.09375
- down_weight: bfloat16 [8, 2048, 7168], P('expert', None, 'dp'), may hold values from -0.125 to 0.125
- shared_gate: bfloat16 [7168, 2048], P('dp'), may hold values from -0.09375 to 0.09375
- shared_up: bfloat16 [7168, 2048], P('dp'), may hold values from -0.09375 to 0.09375
- shared_down: bfloat16 [2048, 7168], P(None, 'dp'), may hold values from -0.125 to 0.125
Outputs:
- mixed: bfloat16 [128, 7168], P('expert', 'dp')
The draws below stay inside these ranges and needn't reach their ends.
Inputs may be any that keep to these rules, and one draw needn't show every extreme that they name: `expert_ids`: each row names 4 different experts. In each aligned block of 16 rows (the tokens of one index of the expert axis) no expert is named by more than 12 rows, and in at least one such block some expert is named by exactly 12 rows.
All inputs are finite; a program needn't handle non-finite values.
Results may differ from the reference program's by a relative error of at most 0.035.
Values may be sent and summed in bfloat16 or wider, within the bound.
A program may use at most 128 MiB of HBM per device.

```python
import math
import jax
import jax.numpy as jnp
import numpy as np
from jax import lax

D = 7168
H = 2048
TOK_DEV = 16
EXPERTS = 8
TOP = 4
CAP = 12
TOKENS = 128
N_DP = 4
N_EXPERT = 8


def strengthened(array, own_key, source, target, parts, factor):
    owner, partner = [(jnp.arange(array.shape[dim]) // (array.shape[dim] // parts)).reshape([-1 if axis == dim else 1 for axis in range(array.ndim)]) for dim in (source, target)]
    chosen = jax.random.permutation(own_key, parts)[partner]
    strong = (owner == chosen) | (owner == (partner + parts // 2) % parts)
    return jnp.where(strong, factor * array, array)


def shard_levels(key, shape, cuts, least, top_value):
    factor_of, own = 1.0, jax.random.fold_in(key, 6)
    for position, blocks in cuts:
        heights = jnp.exp(jax.random.uniform(jax.random.fold_in(own, position), (blocks,), jnp.float32, least / len(cuts), top_value / len(cuts)))
        factor_of = factor_of * jnp.repeat(heights, shape[position] // blocks).reshape([-1 if axis == position else 1 for axis in range(len(shape))])
    return factor_of


def routed_block(own_key, own, number, rows, amount, top, bound, skew):
    sequence = jax.random.permutation(own_key, amount)
    crowded, common = portions_of(amount, rows * top, bound, skew, True), portions_of(amount, rows * top, bound, skew, False)
    places = jnp.arange(amount)

    def named(tallies, offset_by):
        used = int((tallies > 0).sum())
        fixed = max(1, used // 4)
        shifted = fixed + (places - fixed + offset_by * (used - fixed)) % max(1, amount - fixed)
        return jnp.zeros((amount,), jnp.int32).at[sequence[jnp.where(places < fixed, places, shifted)]].set(jnp.asarray(tallies, jnp.int32))

    tallies = jnp.where(number % 4 == 0, named(crowded, number // 4), named(common, number - number // 4 - 1))
    mixed = jax.random.permutation(jax.random.fold_in(own, 3), amount)
    donor, taker = mixed[0:amount // 2 * 2:2], mixed[1:amount // 2 * 2:2]
    slack = jnp.minimum(tallies[donor] - 1, bound - tallies[taker]) // 2
    slack = jnp.where((donor == sequence[0]) | (taker == sequence[0]) | (tallies[taker] == 0), 0, jnp.maximum(slack, 0))
    shifted = jax.random.randint(jax.random.fold_in(own, 4), (amount // 2,), 0, 1 << 20) % (slack + 1)
    tallies = tallies.at[donor].add(-shifted).at[taker].add(shifted)
    labels = jnp.searchsorted(jnp.cumsum(tallies), jnp.arange(rows * top), side="right").astype(jnp.int32)
    listing = labels.reshape(top, rows).T
    listing = listing[jax.random.permutation(jax.random.fold_in(own, 1), rows)]
    offset_by = jax.random.randint(jax.random.fold_in(own, 2), (rows, 1), 0, top)
    return jnp.take_along_axis(listing, (jnp.arange(top)[None, :] + offset_by) % top, axis=1)


def portions_of(number_of, total, reach, skew, full):
    loads = [(1 << 20) // math.isqrt(grade ** skew) + 1 for grade in range(1, number_of + 1)]
    largest = reach if full else min(reach, max(-(-total // number_of), total * loads[0] // sum(loads)))
    least = 1 if total - largest >= number_of - 1 else 0
    given, surplus = [largest] + [least] * (number_of - 1), total - largest - least * (number_of - 1)
    while surplus > 0:
        movable = [i for i in range(1, number_of) if given[i] < largest] or [i for i in range(1, number_of) if given[i] < reach]
        mass, remaining = sum([loads[i] for i in movable]), surplus
        for i in movable:
            extra = min(reach - given[i], max(1, remaining * loads[i] // mass), surplus)
            given[i] = given[i] + extra
            surplus = surplus - extra
    return np.array(given)


def bell_draw(own_key, shape, spread, most, cuts=(), kind=jnp.bfloat16):
    gain = shard_levels(own_key, shape, cuts, -0.22, 0.18) if cuts else 1.0
    entries = jax.random.normal(own_key, shape, jnp.float32) * spread * gain
    return jnp.minimum(jnp.maximum(entries, -most), most).astype(kind)


def bell_draw_with(rng, shape, width, bound, cuts, heavy, kind=jnp.bfloat16):
    array = width * jax.random.normal(rng, shape, jnp.float32)
    if cuts:
        array = array * shard_levels(rng, shape, cuts, -0.22, 0.18)
    return jnp.clip(strengthened(array, jax.random.fold_in(rng, 3), *heavy), -bound, bound).astype(kind)


def setup_inputs(seed: int = 0) -> dict:
    key_list = jax.random.split(jax.random.key(seed), 11)
    shortcut_in = bell_draw(key_list[0], (TOKENS, D), 1.0, 6.0, ((0, 8), (1, 4)))
    current_in = bell_draw(key_list[1], (TOKENS, D), 1.0, 6.0, ((0, 8), (1, 4)))
    expert_ids_keys = jax.random.split(jax.random.fold_in(key_list[2], 1), TOKENS // TOK_DEV)
    expert_ids_turns = jax.random.permutation(jax.random.fold_in(key_list[2], 3), TOKENS // TOK_DEV)
    expert_ids = jax.vmap(lambda own, number: routed_block(jax.random.fold_in(key_list[2], 2), own, number, TOK_DEV, EXPERTS, TOP, CAP, 2))(expert_ids_keys, expert_ids_turns).reshape((TOKENS, TOP))
    route_weight = jnp.clip(jnp.exp(math.log(1.0) - 2.3025851 * jax.random.uniform(key_list[3], (TOKENS, TOP), jnp.float32) ** shard_levels(key_list[3], (TOKENS, TOP), ((0, 8),), -0.2, 0.2)), 0.1, 1.0)
    gate_weight = bell_draw_with(key_list[4], (EXPERTS, D, H), D ** -0.5, 0.09375, ((0, 8), (1, 4)), (1, 2, 4, 2.0))
    up_weight = bell_draw_with(key_list[5], (EXPERTS, D, H), D ** -0.5, 0.09375, ((0, 8), (1, 4)), (1, 2, 4, 2.0))
    down_weight = bell_draw(key_list[6], (EXPERTS, H, D), H ** -0.5, 0.125, ((0, 8), (2, 4)))
    shared_gate = bell_draw_with(key_list[7], (D, H), D ** -0.5, 0.09375, ((0, 4),), (0, 1, 4, 2.0))
    shared_up = bell_draw_with(key_list[8], (D, H), D ** -0.5, 0.09375, ((0, 4),), (0, 1, 4, 2.0))
    shared_down = bell_draw(key_list[9], (H, D), H ** -0.5, 0.125, ((1, 4),))
    return {"shortcut_in": shortcut_in, "current_in": current_in, "expert_ids": expert_ids, "route_weight": route_weight, "gate_weight": gate_weight, "up_weight": up_weight, "down_weight": down_weight, "shared_gate": shared_gate, "shared_up": shared_up, "shared_down": shared_down}


def blocked_product(inputs, weight):
    count = inputs.shape[0]
    block = inputs.shape[1] // N_DP
    pieces = inputs.astype(jnp.float32).reshape(count, N_DP, block)
    blocks = weight.astype(jnp.float32).reshape(N_DP, block, weight.shape[1])
    partial_value = jnp.einsum("rnd,ndh->nrh", pieces, blocks, precision=lax.Precision.HIGHEST)
    rounded = lax.optimization_barrier(partial_value.astype(jnp.bfloat16))
    return jnp.sum(rounded.astype(jnp.float32), axis=0)


def swiglu_hidden(inputs, gate_w, up_w):
    gate = blocked_product(inputs, gate_w)
    upper = blocked_product(inputs, up_w)
    return (jax.nn.silu(gate) * upper).astype(jnp.bfloat16)


def reference(shortcut_in, current_in, expert_ids, route_weight, gate_weight, up_weight, down_weight, shared_gate, shared_up, shared_down):
    count = TOKENS * TOP
    limit = N_EXPERT * CAP
    flat_ids = expert_ids.reshape(-1).astype(jnp.int32)
    flat_tok = jnp.arange(count, dtype=jnp.int32) // TOP
    flat_weight = route_weight.reshape(-1)

    def one_expert(total, inputs):
        gate_w, up_w, down_w, number = inputs
        chosen = flat_ids == number
        rank = jnp.cumsum(chosen.astype(jnp.int32)) - 1
        slots = jnp.where(chosen, rank, limit).astype(jnp.int32)
        source = jnp.zeros((limit,), jnp.int32).at[slots].set(jnp.arange(count, dtype=jnp.int32), mode="drop")
        used = jnp.zeros((limit,), jnp.float32).at[slots].set(1.0, mode="drop")
        token_index = flat_tok[source]
        gathered = shortcut_in[token_index]
        hidden = swiglu_hidden(gathered, gate_w, up_w)
        result = jnp.dot(hidden, down_w, preferred_element_type=jnp.float32).astype(jnp.bfloat16)
        result = lax.optimization_barrier(result).astype(jnp.float32)
        scale = used * flat_weight[source]
        total = total.at[token_index].add(scale[:, None] * result)
        return total, None

    numbers = jnp.arange(EXPERTS, dtype=jnp.int32)
    start = jnp.zeros((TOKENS, D), jnp.float32)
    routed, unused_out = lax.scan(one_expert, start, (gate_weight, up_weight, down_weight, numbers))
    shared_hidden = swiglu_hidden(current_in, shared_gate, shared_up)
    shared_out = jnp.dot(shared_hidden, shared_down, preferred_element_type=jnp.float32)
    return (shared_out + routed).astype(jnp.bfloat16)
```

```python
import functools

import jax
import jax.numpy as jnp
from jax import lax
from jax.experimental import pallas as pl
from jax.experimental.pallas import tpu as pltpu
from jax.sharding import PartitionSpec as P


def activate(summed):
    return (jax.nn.silu(summed[:, 0]) * summed[:, 1]).astype(jnp.bfloat16)


def hidden_of(partial_value):
    summed = lax.psum_scatter(
        partial_value.astype(jnp.bfloat16), "dp", scatter_dimension=2, tiled=True
    ).astype(jnp.float32)
    return lax.all_gather(activate(summed), "dp", axis=1, tiled=True)


def send_rows(outgoing):
    return lax.all_to_all(outgoing, "expert", split_axis=0, concat_axis=0, tiled=True)


def expert_partial(arrived, gate_weight, up_weight):
    gate = jnp.einsum("sacd,adh->sach", arrived, gate_weight, preferred_element_type=jnp.float32)
    upper = jnp.einsum("sacd,adh->sach", arrived, up_weight, preferred_element_type=jnp.float32)
    stacked = jnp.stack([gate, upper], axis=3)
    return stacked.reshape(-1, 2, gate_weight.shape[2])


def local(
    shortcut_in,
    current_in,
    expert_ids,
    route_weight,
    gate_weight,
    up_weight,
    down_weight,
    shared_gate,
    shared_up,
    shared_down,
):
    sources = lax.axis_size("expert")
    local_experts = gate_weight.shape[0]
    experts = sources * local_experts
    tokens, top = expert_ids.shape
    capacity = 3 * tokens * top // (2 * experts)
    width = shortcut_in.shape[1]
    hidden_units = gate_weight.shape[2]
    flat_ids = expert_ids.reshape(-1)
    onehot = (flat_ids[:, None] == jnp.arange(experts, dtype=jnp.int32)[None, :]).astype(jnp.int32)
    rank = jnp.sum((jnp.cumsum(onehot, axis=0) - 1) * onehot, axis=1)
    slot = (flat_ids * capacity + rank).reshape(tokens, top)
    positions = jnp.arange(experts * capacity, dtype=jnp.int32)
    place = jnp.sum((slot[None, :, :] == positions[:, None, None]).astype(jnp.bfloat16), axis=2)
    outgoing = jnp.dot(place, shortcut_in, preferred_element_type=jnp.float32).astype(jnp.bfloat16)
    outgoing = outgoing.reshape(sources, local_experts * capacity, width)
    shared_gate_sum = jnp.dot(current_in, shared_gate, preferred_element_type=jnp.float32)
    shared_up_sum = jnp.dot(current_in, shared_up, preferred_element_type=jnp.float32)
    shared_partial = jnp.stack([shared_gate_sum, shared_up_sum], axis=1)
    routed_rows = experts * capacity
    arrived = send_rows(outgoing).reshape(sources, local_experts, capacity, width)
    routed_partial = expert_partial(arrived, gate_weight, up_weight)
    joined = hidden_of(jnp.concatenate([routed_partial, shared_partial], axis=0))
    routed_hidden = joined[:routed_rows]
    shared_hidden = joined[routed_rows:]
    routed_hidden = routed_hidden.reshape(sources, local_experts, capacity, hidden_units)
    expert_out = jnp.einsum(
        "sach,ahd->sacd", routed_hidden, down_weight, preferred_element_type=jnp.float32
    ).astype(jnp.bfloat16)
    returned = lax.all_to_all(
        expert_out.reshape(sources, local_experts * capacity, width),
        "expert",
        split_axis=0,
        concat_axis=0,
        tiled=True,
    )
    picked = returned.reshape(routed_rows, width)[slot]
    routed = jnp.sum(route_weight[:, :, None] * picked.astype(jnp.float32), axis=1)
    shared_out = jnp.dot(shared_hidden, shared_down, preferred_element_type=jnp.float32)
    return (shared_out + routed).astype(jnp.bfloat16)


MESH = pl.DeviceIdType.MESH
BF = jnp.bfloat16
F32 = jnp.float32
PARTS = 2


def dot(a, b):
    return jnp.dot(a, b, preferred_element_type=F32)


def layer_kernel(
    n_dp, n_e, rows,
    x_ref, cur_ref, ids_ref, w_ref, gate_hbm, up_hbm, down_hbm, sg_hbm, su_hbm, sd_hbm,
    out_ref,
    gate_v, up_v, down_v, sg_v, su_v, sd_v,
    m_own, m_all, x_all, c_all, xc, part, rs_in, hid, acc,
    sh_part, sh_in, sh_hid, contrib, pair_in, fin_out, fin_in,
    gate_sem, up_sem, down_sem, shw_sem,
    m_s, m_r, x_s, x_r, c_s, c_r, mp_s, mp_r, xp_s, xp_r, cp_s, cp_r,
    rs_s, rs_r, hid_s, hid_r, shp_s, shp_r, shh_s, shh_r, pair_s, pair_r, fin_s, fin_r,
):
    me_d = lax.axis_index("dp")
    me_e = lax.axis_index("expert")
    zs = n_e // 2
    z, c = me_e // 2, lax.rem(me_e, 2)
    partner = 2 * z + (1 - c)
    tokens, width = x_ref.shape
    chunk = gate_v.shape[2]
    hs = chunk * PARTS
    total = n_e * tokens
    sh = sg_v.shape[1]
    share = total // n_dp
    slots = [(q, s) for q in range(PARTS) for s in [*range(1, n_dp), 0]]

    def start(copy):
        copy.start()
        return copy

    def dp_dev(s):
        return lax.rem(me_d + s, n_dp)

    def dp_src(s):
        return lax.rem(me_d - s + n_dp, n_dp)

    def z_dev(s):
        return 2 * lax.rem(z + s, zs) + c

    def z_src(s):
        return 2 * lax.rem(z - s + zs, zs) + c

    local_waits = {}
    for i, (q, s) in enumerate(slots):
        col = pl.ds(pl.multiple_of(dp_dev(s) * hs + q * chunk, 128), chunk)
        local_waits["g", q, s] = start(pltpu.make_async_copy(gate_hbm.at[0, :, col], gate_v.at[i], gate_sem.at[i]))
        local_waits["u", q, s] = start(pltpu.make_async_copy(up_hbm.at[0, :, col], up_v.at[i], up_sem.at[i]))
    own = pl.ds(pl.multiple_of(me_e * sh, 128), sh)
    local_waits["sg"] = start(pltpu.make_async_copy(sg_hbm.at[:, own], sg_v, shw_sem.at[0]))
    local_waits["su"] = start(pltpu.make_async_copy(su_hbm.at[:, own], su_v, shw_sem.at[1]))
    local_waits["sd"] = start(pltpu.make_async_copy(sd_hbm.at[own, :], sd_v, shw_sem.at[2]))
    for i, (q, s) in enumerate(slots):
        row = pl.ds(pl.multiple_of(dp_src(s) * hs + q * chunk, 128), chunk)
        local_waits["d", q, s] = start(pltpu.make_async_copy(down_hbm.at[0, row, :], down_v.at[i], down_sem.at[i]))

    barrier = pltpu.get_barrier_semaphore()
    for s in range(1, n_dp):
        pl.semaphore_signal(barrier, inc=1, device_id=(dp_dev(s), me_e), device_id_type=MESH)
    for s in range(1, zs):
        pl.semaphore_signal(barrier, inc=1, device_id=(me_d, z_dev(s)), device_id_type=MESH)
    pl.semaphore_signal(barrier, inc=1, device_id=(me_d, partner), device_id_type=MESH)

    lanes = lax.broadcasted_iota(jnp.int32, (tokens, 128), 1)
    ids, weight = ids_ref[...], w_ref[...]
    mine = jnp.zeros((tokens, 128), F32)
    for k in range(ids.shape[1]):
        mine += jnp.where(ids[:, k:k + 1] == lanes, weight[:, k:k + 1], 0.0)
    m_own[...] = mine
    m_all[me_e] = mine
    x_all[me_e] = x_ref[...]
    c_all[me_e] = cur_ref[...]
    pl.semaphore_wait(barrier, n_dp - 1 + zs - 1 + 1)

    sends = []

    def remote(src, dst, ssem, rsem, dp, e):
        copy = pltpu.make_async_remote_copy(
            src_ref=src, dst_ref=dst, send_sem=ssem, recv_sem=rsem, device_id=(dp, e), device_id_type=MESH
        )
        copy.start()
        sends.append(copy)

    def arrived(dst, ssem, rsem):
        pltpu.make_async_remote_copy(
            src_ref=dst, dst_ref=dst, send_sem=ssem, recv_sem=rsem, device_id=(me_d, partner), device_id_type=MESH
        ).wait_recv()

    groups = [(m_own, m_all, m_s, m_r, mp_s, mp_r), (x_ref, x_all, x_s, x_r, xp_s, xp_r), (cur_ref, c_all, c_s, c_r, cp_s, cp_r)]

    def spread(src, buf, ss, rr, ps, pr):
        for s in range(zs - 1, 0, -1):
            remote(src, buf.at[me_e], ss.at[s], rr.at[s], me_d, z_dev(s))
        remote(src, buf.at[me_e], ps.at[0], pr.at[0], me_d, partner)

    def relay(src, buf, ss, rr, ps, pr):
        for s in range(1, zs):
            block = buf.at[z_src(s)]
            arrived(block, ss.at[s], rr.at[s])
            remote(block, block, ps.at[s], pr.at[s], me_d, partner)

    def collect(src, buf, ss, rr, ps, pr):
        for s in range(zs):
            arrived(buf.at[z_src(s) + 1 - 2 * c], ps.at[s], pr.at[s])

    spread(*groups[0])
    spread(*groups[1])
    relay(*groups[0])
    collect(*groups[0])
    routing = m_all[...].reshape(total, 128)
    named = jnp.where(routing > 0, 1.0, 0.0)
    below = lax.broadcasted_iota(jnp.int32, (total, total), 1) < lax.broadcasted_iota(jnp.int32, (total, total), 0)
    rank = dot(jnp.where(below, 1.0, 0.0).astype(BF), named.astype(BF))
    pick = lax.broadcasted_iota(jnp.int32, (total, 128), 1) == me_e
    rank_col = jnp.sum(jnp.where(pick, rank, 0.0), axis=1, keepdims=True)
    scale_col = jnp.sum(jnp.where(pick, routing, 0.0), axis=1, keepdims=True)
    padded = -(-rows // 128) * 128
    slot = lax.broadcasted_iota(jnp.int32, (total, padded), 1).astype(F32)
    placed_t = jnp.where(jnp.logical_and(slot == rank_col, scale_col > 0), 1.0, 0.0)
    gather = jnp.transpose(placed_t)[:rows].astype(BF)
    scatter = placed_t.astype(BF)[:, :rows]

    relay(*groups[1])
    spread(*groups[2])
    collect(*groups[1])
    xc[...] = dot(gather, x_all[...].reshape(total, width)).astype(BF)

    for i, (q, s) in enumerate(slots):
        local_waits["g", q, s].wait()
        local_waits["u", q, s].wait()
        part[i, :, :chunk] = dot(xc[...], gate_v[i]).astype(BF)
        part[i, :, chunk:] = dot(xc[...], up_v[i]).astype(BF)
        if s:
            remote(part.at[i], rs_in.at[i], rs_s.at[i], rs_r.at[i], dp_dev(s), me_e)

    relay(*groups[2])
    collect(*groups[2])
    local_waits["sg"].wait()
    local_waits["su"].wait()
    cur = c_all[...].reshape(total, width)
    sh_part[:, :, :sh] = dot(cur, sg_v[...]).astype(BF).reshape(n_dp, share, sh)
    sh_part[:, :, sh:] = dot(cur, su_v[...]).astype(BF).reshape(n_dp, share, sh)
    for s in range(1, n_dp):
        remote(sh_part.at[dp_dev(s)], sh_in.at[s], shp_s.at[s], shp_r.at[s], dp_dev(s), me_e)

    def act(term, n):
        gate, upper = term[:, :n], term[:, n:]
        return (gate / (1.0 + jnp.exp(-gate)) * upper).astype(BF)

    def routed_act(q):
        base = q * n_dp
        term = part[base + n_dp - 1].astype(F32)
        for s in range(1, n_dp):
            i = base + s - 1
            arrived(rs_in.at[i], rs_s.at[i], rs_r.at[i])
            term = term + rs_in[i].astype(F32)
        j = base + n_dp - 1
        hid[j] = act(term, chunk)
        for s in range(1, n_dp):
            i = base + s - 1
            remote(hid.at[j], hid.at[i], hid_s.at[i], hid_r.at[i], dp_dev(s), me_e)

    def routed_down(q, first):
        base = q * n_dp
        for s in [0, *range(1, n_dp)]:
            i = base + (s - 1 if s else n_dp - 1)
            if s:
                arrived(hid.at[i], hid_s.at[i], hid_r.at[i])
            local_waits["d", q, s].wait()
            value = dot(hid[i], down_v[i])
            acc[...] = value if first and s == 0 else acc[...] + value

    for q in range(PARTS):
        routed_act(q)
    term = sh_part[me_d].astype(F32)
    for s in range(1, n_dp):
        arrived(sh_in.at[s], shp_s.at[s], shp_r.at[s])
        term = term + sh_in[s].astype(F32)
    sh_hid[me_d] = act(term, sh)
    for s in range(1, n_dp):
        remote(sh_hid.at[me_d], sh_hid.at[me_d], shh_s.at[s], shh_r.at[s], dp_dev(s), me_e)
    for q in range(PARTS):
        routed_down(q, q == 0)
    for s in range(1, n_dp):
        arrived(sh_hid.at[dp_src(s)], shh_s.at[s], shh_r.at[s])
    local_waits["sd"].wait()
    value = dot(sh_hid[...].reshape(total, sh), sd_v[...])
    value = value + scale_col * dot(scatter, acc[...].astype(BF))
    contrib[...] = value.astype(BF).reshape(n_e, tokens, width)
    order = [*range(zs - 1, -1, -1)]
    for s in order:
        remote(contrib.at[2 * lax.rem(z + s, zs) + 1 - c], pair_in.at[s], pair_s.at[s], pair_r.at[s], me_d, partner)
    for s in order:
        arrived(pair_in.at[s], pair_s.at[s], pair_r.at[s])
        both = contrib[z_dev(s)].astype(F32) + pair_in[s].astype(F32)
        if s:
            fin_out[s] = both.astype(BF)
            remote(fin_out.at[s], fin_in.at[s], fin_s.at[s], fin_r.at[s], me_d, z_dev(s))
    for s in range(1, zs):
        arrived(fin_in.at[s], fin_s.at[s], fin_r.at[s])
        both = both + fin_in[s].astype(F32)
    out_ref[...] = both.astype(BF)
    for copy in sends:
        copy.wait_send()


def fused(n_dp, n_e, shortcut_in, current_in, expert_ids, route_weight, gate_weight, up_weight, down_weight, shared_gate, shared_up, shared_down):
    tokens, width = shortcut_in.shape
    hidden = gate_weight.shape[2]
    top = expert_ids.shape[1]
    capacity = 3 * tokens * top // (2 * n_e)
    rows = min(-(-capacity * n_e // 16) * 16, n_e * tokens)
    chunk = hidden // n_dp // PARTS
    count = PARTS * n_dp
    sh = hidden // n_e
    zs = n_e // 2
    total = n_e * tokens
    share = total // n_dp
    V = pltpu.VMEM
    S = pltpu.SemaphoreType.DMA
    scratch = [
        V((count, width, chunk), BF), V((count, width, chunk), BF), V((count, chunk, width), BF),
        V((width, sh), BF), V((width, sh), BF), V((sh, width), BF),
        V((tokens, 128), F32), V((n_e, tokens, 128), F32), V((n_e, tokens, width), BF), V((n_e, tokens, width), BF),
        V((rows, width), BF), V((count, rows, 2 * chunk), BF), V((count, rows, 2 * chunk), BF),
        V((count, rows, chunk), BF), V((rows, width), F32),
        V((n_dp, share, 2 * sh), BF), V((n_dp, share, 2 * sh), BF), V((n_dp, share, sh), BF),
        V((n_e, tokens, width), BF), V((zs, tokens, width), BF), V((zs, tokens, width), BF), V((zs, tokens, width), BF),
        S((count,)), S((count,)), S((count,)), S((3,)),
        *[S((zs,)) for _ in range(12)],
        *[S((count,)) for _ in range(4)],
        *[S((n_dp,)) for _ in range(4)],
        *[S((zs,)) for _ in range(4)],
    ]
    vm = pl.BlockSpec(memory_space=pltpu.VMEM)
    hbm = pl.BlockSpec(memory_space=pl.ANY)
    return pl.pallas_call(
        functools.partial(layer_kernel, n_dp, n_e, rows),
        out_shape=jax.ShapeDtypeStruct((tokens, width), BF),
        in_specs=[vm] * 4 + [hbm] * 6,
        out_specs=vm,
        scratch_shapes=scratch,
        compiler_params=pltpu.CompilerParams(collective_id=0, has_side_effects=True, vmem_limit_bytes=60 * 1024 * 1024),
    )(shortcut_in, current_in, expert_ids, route_weight, gate_weight, up_weight, down_weight, shared_gate, shared_up, shared_down)


def body(n_dp, n_e, *arrays):
    tokens, width = arrays[0].shape
    experts, _, hidden = arrays[4].shape
    aligned = (
        experts == 1 and n_e % 2 == 0 and n_e <= 128 and tokens % 16 == 0 and width % 128 == 0
        and hidden % (n_dp * PARTS * 128) == 0 and hidden % (n_e * 128) == 0
        and n_e * tokens % (n_dp * 16) == 0
    )
    return fused(n_dp, n_e, *arrays) if aligned else local(*arrays)


def solution(mesh):
    placed = (
        P("expert", "dp"),
        P("expert", "dp"),
        P("expert", None),
        P("expert", None),
        P("expert", "dp", None),
        P("expert", "dp", None),
        P("expert", None, "dp"),
        P("dp", None),
        P("dp", None),
        P(None, "dp"),
    )
    return jax.shard_map(
        functools.partial(body, mesh.shape["dp"], mesh.shape["expert"]), mesh=mesh, in_specs=placed, out_specs=P("expert", "dp"), check_vma=False
    )
```

```python
import functools

import jax
import jax.numpy as jnp
from jax import lax
from jax.experimental import pallas as pl
from jax.experimental.pallas import tpu as pltpu
from jax.sharding import PartitionSpec as P


def activate(summed):
    return (jax.nn.silu(summed[:, 0]) * summed[:, 1]).astype(jnp.bfloat16)


def hidden_of(partial_value):
    summed = lax.psum_scatter(
        partial_value.astype(jnp.bfloat16), "dp", scatter_dimension=2, tiled=True
    ).astype(jnp.float32)
    return lax.all_gather(activate(summed), "dp", axis=1, tiled=True)


def send_rows(outgoing):
    return lax.all_to_all(outgoing, "expert", split_axis=0, concat_axis=0, tiled=True)


def expert_partial(arrived, gate_weight, up_weight):
    gate = jnp.einsum("sacd,adh->sach", arrived, gate_weight, preferred_element_type=jnp.float32)
    upper = jnp.einsum("sacd,adh->sach", arrived, up_weight, preferred_element_type=jnp.float32)
    stacked = jnp.stack([gate, upper], axis=3)
    return stacked.reshape(-1, 2, gate_weight.shape[2])


def local(
    shortcut_in,
    current_in,
    expert_ids,
    route_weight,
    gate_weight,
    up_weight,
    down_weight,
    shared_gate,
    shared_up,
    shared_down,
):
    sources = lax.axis_size("expert")
    local_experts = gate_weight.shape[0]
    experts = sources * local_experts
    tokens, top = expert_ids.shape
    capacity = 3 * tokens * top // (2 * experts)
    width = shortcut_in.shape[1]
    hidden_units = gate_weight.shape[2]
    flat_ids = expert_ids.reshape(-1)
    onehot = (flat_ids[:, None] == jnp.arange(experts, dtype=jnp.int32)[None, :]).astype(jnp.int32)
    rank = jnp.sum((jnp.cumsum(onehot, axis=0) - 1) * onehot, axis=1)
    slot = (flat_ids * capacity + rank).reshape(tokens, top)
    positions = jnp.arange(experts * capacity, dtype=jnp.int32)
    place = jnp.sum((slot[None, :, :] == positions[:, None, None]).astype(jnp.bfloat16), axis=2)
    outgoing = jnp.dot(place, shortcut_in, preferred_element_type=jnp.float32).astype(jnp.bfloat16)
    outgoing = outgoing.reshape(sources, local_experts * capacity, width)
    shared_gate_sum = jnp.dot(current_in, shared_gate, preferred_element_type=jnp.float32)
    shared_up_sum = jnp.dot(current_in, shared_up, preferred_element_type=jnp.float32)
    shared_partial = jnp.stack([shared_gate_sum, shared_up_sum], axis=1)
    routed_rows = experts * capacity
    arrived = send_rows(outgoing).reshape(sources, local_experts, capacity, width)
    routed_partial = expert_partial(arrived, gate_weight, up_weight)
    joined = hidden_of(jnp.concatenate([routed_partial, shared_partial], axis=0))
    routed_hidden = joined[:routed_rows]
    shared_hidden = joined[routed_rows:]
    routed_hidden = routed_hidden.reshape(sources, local_experts, capacity, hidden_units)
    expert_out = jnp.einsum(
        "sach,ahd->sacd", routed_hidden, down_weight, preferred_element_type=jnp.float32
    ).astype(jnp.bfloat16)
    returned = lax.all_to_all(
        expert_out.reshape(sources, local_experts * capacity, width),
        "expert",
        split_axis=0,
        concat_axis=0,
        tiled=True,
    )
    picked = returned.reshape(routed_rows, width)[slot]
    routed = jnp.sum(route_weight[:, :, None] * picked.astype(jnp.float32), axis=1)
    shared_out = jnp.dot(shared_hidden, shared_down, preferred_element_type=jnp.float32)
    return (shared_out + routed).astype(jnp.bfloat16)


MESH = pl.DeviceIdType.MESH
BF = jnp.bfloat16
F32 = jnp.float32
PARTS = 2


def dot(a, b):
    return jnp.dot(a, b, preferred_element_type=F32)


def layer_kernel(
    n_dp, n_e, rows,
    x_ref, cur_ref, ids_ref, w_ref, gate_hbm, up_hbm, down_hbm, sg_hbm, su_hbm, sd_hbm,
    out_ref,
    gate_v, up_v, down_v, sg_v, su_v, sd_v,
    flip, m_own, m_all, x_all, c_all, xc, part, rs_in, hid, acc, shv,
    sh_part, sh_in, sh_hid, own_sum, contrib, pair_in, fin_out, fin_in,
    gate_sem, up_sem, down_sem, shw_sem,
    m_s, m_r, x_s, x_r, c_s, c_r, mp_s, mp_r, xp_s, xp_r, cp_s, cp_r,
    rs_s, rs_r, hid_s, hid_r, shp_s, shp_r, shh_s, shh_r, pair_s, pair_r, fin_s, fin_r,
):
    me_d = lax.axis_index("dp")
    me_e = lax.axis_index("expert")
    zs = n_e // 2
    z, c = me_e // 2, lax.rem(me_e, 2)
    pairs = zs // 2
    p, b = z // 2, lax.rem(z, 2)
    partner = 2 * z + (1 - c)
    tokens, width = x_ref.shape
    chunk = gate_v.shape[2]
    hs = chunk * PARTS
    total = n_e * tokens
    sh = sg_v.shape[1]
    share = total // n_dp
    slots = [(q, s) for q in range(PARTS) for s in [*range(1, n_dp), 0]]

    def start(copy):
        copy.start()
        return copy

    def dp_dev(s):
        return lax.rem(me_d + s, n_dp)

    def dp_src(s):
        return lax.rem(me_d - s + n_dp, n_dp)

    def z_dev(s):
        return 2 * (2 * lax.rem(p + s // 2, pairs) + lax.rem(b + s % 2, 2)) + c

    def z_src(s):
        return 2 * (2 * lax.rem(p - s // 2 + pairs, pairs) + lax.rem(b + s % 2, 2)) + c

    def group_blocks(a):
        return pl.ds(4 * lax.rem(p - a + pairs, pairs), 4)

    local_waits = {}
    for i, (q, s) in enumerate(slots):
        col = pl.ds(pl.multiple_of(dp_dev(s) * hs + q * chunk, 128), chunk)
        local_waits["g", q, s] = start(pltpu.make_async_copy(gate_hbm.at[0, :, col], gate_v.at[i], gate_sem.at[i]))
        local_waits["u", q, s] = start(pltpu.make_async_copy(up_hbm.at[0, :, col], up_v.at[i], up_sem.at[i]))
    own = pl.ds(pl.multiple_of(me_e * sh, 128), sh)
    local_waits["sg"] = start(pltpu.make_async_copy(sg_hbm.at[:, own], sg_v, shw_sem.at[0]))
    local_waits["su"] = start(pltpu.make_async_copy(su_hbm.at[:, own], su_v, shw_sem.at[1]))
    local_waits["sd"] = start(pltpu.make_async_copy(sd_hbm.at[own, :], sd_v, shw_sem.at[2]))
    for i, (q, s) in enumerate(slots):
        row = pl.ds(pl.multiple_of(dp_src(s) * hs + q * chunk, 128), chunk)
        local_waits["d", q, s] = start(pltpu.make_async_copy(down_hbm.at[0, row, :], down_v.at[i], down_sem.at[i]))

    barrier = pltpu.get_barrier_semaphore()
    for s in range(1, n_dp):
        pl.semaphore_signal(barrier, inc=1, device_id=(dp_dev(s), me_e), device_id_type=MESH)
    for s in range(1, zs):
        pl.semaphore_signal(barrier, inc=1, device_id=(me_d, z_dev(s)), device_id_type=MESH)
    pl.semaphore_signal(barrier, inc=1, device_id=(me_d, partner), device_id_type=MESH)

    top = ids_ref.shape[0]
    flip[...] = jnp.zeros_like(flip)
    flip[:top, :tokens] = ids_ref[...].astype(F32)
    flip[top:2 * top, :tokens] = w_ref[...]
    named_ids = lax.broadcasted_iota(jnp.int32, (128, 128), 0).astype(F32)
    table = jnp.zeros((128, 128), F32)
    for k in range(top):
        table += jnp.where(flip[k:k + 1, :] == named_ids, flip[top + k:top + k + 1, :], 0.0)
    mine = jnp.transpose(table)[:tokens]
    m_own[...] = mine
    m_all[me_e] = mine
    x_all[me_e] = x_ref[...]
    c_all[me_e] = cur_ref[...]
    pl.semaphore_wait(barrier, n_dp - 1 + zs - 1 + 1)

    sends = []

    def remote(src, dst, ssem, rsem, dp, e):
        copy = pltpu.make_async_remote_copy(
            src_ref=src, dst_ref=dst, send_sem=ssem, recv_sem=rsem, device_id=(dp, e), device_id_type=MESH
        )
        copy.start()
        sends.append(copy)

    def arrived(dst, ssem, rsem):
        pltpu.make_async_remote_copy(
            src_ref=dst, dst_ref=dst, send_sem=ssem, recv_sem=rsem, device_id=(me_d, partner), device_id_type=MESH
        ).wait_recv()

    groups = [(m_own, m_all, m_s, m_r, mp_s, mp_r), (x_ref, x_all, x_s, x_r, xp_s, xp_r), (cur_ref, c_all, c_s, c_r, cp_s, cp_r)]

    def spread(src, buf, ss, rr, ps, pr):
        remote(src, buf.at[me_e], ps.at[0], pr.at[0], me_d, partner)
        for s in range(1, zs):
            remote(src, buf.at[me_e], ss.at[s], rr.at[s], me_d, z_dev(s))

    def relay(s, src, buf, ss, rr, ps, pr):
        if s:
            block = buf.at[z_src(s)]
            arrived(block, ss.at[s], rr.at[s])
            remote(block, block, ps.at[s], pr.at[s], me_d, partner)

    def collect(s, src, buf, ss, rr, ps, pr):
        arrived(buf.at[z_src(s) + 1 - 2 * c], ps.at[s], pr.at[s])

    spread(*groups[0])
    spread(*groups[1])
    spread(*groups[2])
    held = 4 * tokens
    below = lax.broadcasted_iota(jnp.int32, (held, held), 1) < lax.broadcasted_iota(jnp.int32, (held, held), 0)
    below = jnp.where(below, 1.0, 0.0).astype(BF)
    pick = lax.broadcasted_iota(jnp.int32, (held, 128), 1) == me_e
    padded = -(-rows // 128) * 128
    slot = lax.broadcasted_iota(jnp.int32, (held, padded), 1).astype(F32)
    combine = []
    for a in range(pairs):
        for s in (2 * a, 2 * a + 1):
            relay(s, *groups[0])
        for s in (2 * a, 2 * a + 1):
            relay(s, *groups[1])
        for s in (2 * a, 2 * a + 1):
            collect(s, *groups[0])
        routing = m_all[group_blocks(a)].reshape(held, 128)
        rank = dot(below, jnp.where(routing > 0, 1.0, 0.0).astype(BF))
        rank_col = jnp.sum(jnp.where(pick, rank, 0.0), axis=1, keepdims=True)
        scale_col = jnp.sum(jnp.where(pick, routing, 0.0), axis=1, keepdims=True)
        placed_t = jnp.where(jnp.logical_and(slot == rank_col, scale_col > 0), 1.0, 0.0)
        gather = jnp.transpose(placed_t)[:rows].astype(BF)
        combine.append((placed_t.astype(BF)[:, :rows], scale_col))
        for s in (2 * a, 2 * a + 1):
            collect(s, *groups[1])
        xc[a] = dot(gather, x_all[group_blocks(a)].reshape(held, width)).astype(BF)
        for i, (q, s) in enumerate(slots):
            if a == 0:
                local_waits["g", q, s].wait()
                local_waits["u", q, s].wait()
            n = a * len(slots) + i
            part[n, :, :chunk] = dot(xc[a], gate_v[i]).astype(BF)
            part[n, :, chunk:] = dot(xc[a], up_v[i]).astype(BF)
            if s:
                remote(part.at[n], rs_in.at[n], rs_s.at[n], rs_r.at[n], dp_dev(s), me_e)

    def act(term, n):
        gate, upper = term[:, :n], term[:, n:]
        return (gate / (1.0 + jnp.exp(-gate)) * upper).astype(BF)

    def routed_act(a, q):
        base = a * len(slots) + q * n_dp
        term = part[base + n_dp - 1].astype(F32)
        for s in range(1, n_dp):
            i = base + s - 1
            arrived(rs_in.at[i], rs_s.at[i], rs_r.at[i])
            term = term + rs_in[i].astype(F32)
        j = base + n_dp - 1
        hid[j] = act(term, chunk)
        for s in range(1, n_dp):
            i = base + s - 1
            remote(hid.at[j], hid.at[i], hid_s.at[i], hid_r.at[i], dp_dev(s), me_e)

    def routed_down(a):
        for q in range(PARTS):
            base = q * n_dp
            for s in [0, *range(1, n_dp)]:
                i = base + (s - 1 if s else n_dp - 1)
                n = a * len(slots) + i
                if s:
                    arrived(hid.at[n], hid_s.at[n], hid_r.at[n])
                if a == pairs - 1:
                    local_waits["d", q, s].wait()
                value = dot(hid[n], down_v[i])
                acc[...] = value if q == 0 and s == 0 else acc[...] + value

    for s in range(1, zs):
        relay(s, *groups[2])
    for s in range(zs):
        collect(s, *groups[2])
    local_waits["sg"].wait()
    local_waits["su"].wait()
    cur = c_all[...].reshape(total, width)
    sh_part[:, :, :sh] = dot(cur, sg_v[...]).astype(BF).reshape(n_dp, share, sh)
    sh_part[:, :, sh:] = dot(cur, su_v[...]).astype(BF).reshape(n_dp, share, sh)
    for s in range(1, n_dp):
        remote(sh_part.at[dp_dev(s)], sh_in.at[s], shp_s.at[s], shp_r.at[s], dp_dev(s), me_e)
    for q in range(PARTS):
        routed_act(pairs - 1, q)
    term = sh_part[me_d].astype(F32)
    for s in range(1, n_dp):
        arrived(sh_in.at[s], shp_s.at[s], shp_r.at[s])
        term = term + sh_in[s].astype(F32)
    sh_hid[me_d] = act(term, sh)
    for s in range(1, n_dp):
        remote(sh_hid.at[me_d], sh_hid.at[me_d], shh_s.at[s], shh_r.at[s], dp_dev(s), me_e)

    for a in range(pairs - 2, -1, -1):
        for q in range(PARTS):
            routed_act(a, q)
    for a in range(pairs - 1, -1, -1):
        routed_down(a)
        if a == pairs - 1:
            for s in range(1, n_dp):
                arrived(sh_hid.at[dp_src(s)], shh_s.at[s], shh_r.at[s])
            local_waits["sd"].wait()
            shv[...] = dot(sh_hid[...].reshape(total, sh), sd_v[...]).reshape(n_e, tokens, width)
        scatter, scale_col = combine[a]
        value = scale_col * dot(scatter, acc[...].astype(BF))
        value = value + shv[group_blocks(a)].reshape(held, width)
        contrib[group_blocks(a)] = value.astype(BF).reshape(4, tokens, width)
        for s in (2 * a + 1, 2 * a):
            remote(contrib.at[z_src(s) + 1 - 2 * c], pair_in.at[s], pair_s.at[s], pair_r.at[s], me_d, partner)
        for s in (2 * a + 1, 2 * a):
            arrived(pair_in.at[s], pair_s.at[s], pair_r.at[s])
            summed = contrib[z_src(s)].astype(F32) + pair_in[s].astype(F32)
            if s:
                fin_out[s] = summed.astype(BF)
                remote(fin_out.at[s], fin_in.at[s], fin_s.at[s], fin_r.at[s], me_d, z_src(s))
            else:
                own_sum[...] = summed
    both = own_sum[...]
    for s in range(1, zs):
        arrived(fin_in.at[s], fin_s.at[s], fin_r.at[s])
        both = both + fin_in[s].astype(F32)
    out_ref[...] = both.astype(BF)
    for copy in sends:
        copy.wait_send()


def fused(n_dp, n_e, shortcut_in, current_in, expert_ids, route_weight, gate_weight, up_weight, down_weight, shared_gate, shared_up, shared_down):
    tokens, width = shortcut_in.shape
    hidden = gate_weight.shape[2]
    top = expert_ids.shape[1]
    capacity = 3 * tokens * top // (2 * n_e)
    rows = min(-(-capacity * 4 // 16) * 16, 4 * tokens)
    chunk = hidden // n_dp // PARTS
    count = PARTS * n_dp
    sh = hidden // n_e
    zs = n_e // 2
    pairs = zs // 2
    total = n_e * tokens
    share = total // n_dp
    V = pltpu.VMEM
    S = pltpu.SemaphoreType.DMA
    scratch = [
        V((count, width, chunk), BF), V((count, width, chunk), BF), V((count, chunk, width), BF),
        V((width, sh), BF), V((width, sh), BF), V((sh, width), BF),
        V((-(-2 * top // 8) * 8, 128), F32), V((tokens, 128), F32), V((n_e, tokens, 128), F32), V((n_e, tokens, width), BF), V((n_e, tokens, width), BF),
        V((pairs, rows, width), BF), V((pairs * count, rows, 2 * chunk), BF), V((pairs * count, rows, 2 * chunk), BF),
        V((pairs * count, rows, chunk), BF), V((rows, width), F32), V((n_e, tokens, width), F32),
        V((n_dp, share, 2 * sh), BF), V((n_dp, share, 2 * sh), BF), V((n_dp, share, sh), BF), V((tokens, width), F32),
        V((n_e, tokens, width), BF), V((zs, tokens, width), BF), V((zs, tokens, width), BF), V((zs, tokens, width), BF),
        S((count,)), S((count,)), S((count,)), S((3,)),
        *[S((zs,)) for _ in range(12)],
        *[S((pairs * count,)) for _ in range(4)],
        *[S((n_dp,)) for _ in range(4)],
        *[S((zs,)) for _ in range(4)],
    ]
    vm = pl.BlockSpec(memory_space=pltpu.VMEM)
    hbm = pl.BlockSpec(memory_space=pl.ANY)
    return pl.pallas_call(
        functools.partial(layer_kernel, n_dp, n_e, rows),
        out_shape=jax.ShapeDtypeStruct((tokens, width), BF),
        in_specs=[vm] * 4 + [hbm] * 6,
        out_specs=vm,
        scratch_shapes=scratch,
        compiler_params=pltpu.CompilerParams(collective_id=0, has_side_effects=True, vmem_limit_bytes=60 * 1024 * 1024),
    )(shortcut_in, current_in, expert_ids.T, route_weight.T, gate_weight, up_weight, down_weight, shared_gate, shared_up, shared_down)


def body(n_dp, n_e, *arrays):
    tokens, width = arrays[0].shape
    experts, _, hidden = arrays[4].shape
    aligned = (
        experts == 1 and n_e % 4 == 0 and tokens <= 128 and n_e <= 128 and tokens % 16 == 0 and width % 128 == 0
        and hidden % (n_dp * PARTS * 128) == 0 and hidden % (n_e * 128) == 0
        and n_e * tokens % (n_dp * 16) == 0
    )
    return fused(n_dp, n_e, *arrays) if aligned else local(*arrays)


def solution(mesh):
    placed = (
        P("expert", "dp"),
        P("expert", "dp"),
        P("expert", None),
        P("expert", None),
        P("expert", "dp", None),
        P("expert", "dp", None),
        P("expert", None, "dp"),
        P("dp", None),
        P("dp", None),
        P(None, "dp"),
    )
    return jax.shard_map(
        functools.partial(body, mesh.shape["dp"], mesh.shape["expert"]), mesh=mesh, in_specs=placed, out_specs=P("expert", "dp"), check_vma=False
    )
```
